32 devices in a mesh: slab: 8 (over y, x, core), lev: 4 (over z).
Axes of the slice: x: 2, y: 2, z: 4, core: 2. Of those that a mesh axis runs over, the one named last changes fastest.
Arguments:
- ensemble: float32 [80, 16, 18432], P(None, 'lev', 'slab'), may hold values from -6 to 6
- obs_cell: int32 [2, 256], replicated, may hold values from 0 to 294911, as said below
- obs_value: float32 [2, 256], replicated, may hold values from -6 to 6
- obs_var: float32 [2, 256], replicated, may hold values from 0.3 to 3
- obs_frac: float32 [2, 256], replicated, may hold values from 0 to 1
- loc_column: bfloat16 [2, 256, 18432], P(None, 'lev', 'slab'), may hold values from 0 to 1
- loc_level: float32 [2, 256, 16], P(None, None, 'lev'), may hold values from 0.2 to 1
Outputs:
- analysis: float32 [80, 16, 18432], P(None, 'lev', 'slab')
- prior_mean: float32 [2, 256], replicated
The draws below stay inside these ranges and needn't reach their ends.
Inputs may be any that keep to these rules, and one draw needn't show every extreme that they name: `obs_cell`: in each block, every device's cells (a level band of 4 levels and a slab of 2304 columns) hold at least one observation, and one of them lies in the slab's last column.
All inputs are finite; a program needn't handle non-finite values.
Results may differ from the reference program's by a relative error of at most 0.0055.
Values may be sent and summed in bfloat16 or wider, within the bound.
A program may use at most 64 MiB of HBM per device.

```python
import math
import jax
import jax.numpy as jnp
from jax import lax

MEM = 80
CL = 4
CC = 2304
NOBS = 256
BLOCKS = 2
NL = 16
NC = 18432


def draw_obs_cell(key, part):
    n_slabs = NC // CC
    n_bands = NL // CL
    owners = n_slabs * n_bands
    block_rows = []
    for block_index in range(BLOCKS):
        block_key = jax.random.fold_in(key, 101 + block_index)
        keys = jax.random.split(block_key, 6)
        owner_ids = jax.random.permutation(keys[0], owners).astype(jnp.int32)
        owner_slab = owner_ids % n_slabs
        owner_band = owner_ids // n_slabs
        owner_level = owner_band * CL + jax.random.randint(keys[1], (owners,), 0, CL, dtype=jnp.int32)
        owner_column = owner_slab * CC + CC - 1
        extra = NOBS - owners
        rest_level = jax.random.randint(keys[2], (extra,), 0, NL, dtype=jnp.int32)
        slab_one = jax.random.randint(keys[3], (extra,), 0, n_slabs, dtype=jnp.int32)
        slab_two = jax.random.randint(keys[4], (extra,), 0, n_slabs, dtype=jnp.int32)
        rest_slab = slab_one * slab_two // n_slabs
        rest_column = rest_slab * CC + jax.random.randint(keys[5], (extra,), 0, CC, dtype=jnp.int32)
        levels_all = jnp.concatenate([owner_level, rest_level])
        columns_all = jnp.concatenate([owner_column, rest_column])
        block_rows.append((levels_all * NC + columns_all).astype(jnp.int32))
    return jnp.stack(block_rows)


def steps_of(own_key, dims, cuts, smallest, largest):
    def one(position, shards_of):
        steps = jax.random.uniform(jax.random.fold_in(jax.random.fold_in(own_key, 6), position), (shards_of,), jnp.float32, smallest / len(cuts), largest / len(cuts))
        return jnp.repeat(jnp.exp(steps), dims[position] // shards_of).reshape((-1,) + (1,) * (len(dims) - position - 1))

    factor_of = one(*cuts[0])
    for cut in cuts[1:]:
        factor_of = factor_of * one(*cut)
    return factor_of


def scatter_about(key, shape, scale, reach, cuts=(), kind=jnp.bfloat16):
    gain = steps_of(key, shape, cuts, -0.22, 0.18) if cuts else 1.0
    array = jax.random.normal(key, shape, jnp.float32) * scale * gain
    return jnp.minimum(jnp.maximum(array, -reach), reach).astype(kind)


def setup_inputs(seed: int = 0) -> dict:
    seeds = jax.random.split(jax.random.key(seed), 8)
    ensemble = scatter_about(seeds[0], (MEM, NL, NC), 1.0, 6.0, ((1, 4), (2, 8)), jnp.float32)
    obs_cell = draw_obs_cell(jax.random.fold_in(seeds[7], 71), 0)
    obs_value = scatter_about(seeds[2], (BLOCKS, NOBS), 1.5, 6.0, (), jnp.float32)
    obs_var = jnp.clip(jnp.exp(jax.random.uniform(seeds[3], (BLOCKS, NOBS), jnp.float32, math.log(0.3), math.log(3.0))), 0.3, 3.0)
    obs_frac = jnp.clip(jax.random.uniform(seeds[4], (BLOCKS, NOBS), jnp.float32, 0.0, 1.0), 0.0, 1.0)
    loc_column = jnp.clip(1.0 * jax.random.uniform(seeds[5], (BLOCKS, NOBS, NC), jnp.float32) ** steps_of(seeds[5], (BLOCKS, NOBS, NC), ((1, 4), (2, 8)), -0.2, 0.2), 0.0, 1.0).astype(jnp.bfloat16)
    loc_level = jnp.clip(0.2 + 0.8 * jax.random.uniform(seeds[6], (BLOCKS, NOBS, NL), jnp.float32) ** steps_of(seeds[6], (BLOCKS, NOBS, NL), ((2, 4),), -0.2, 0.2), 0.2, 1.0)
    return dict(ensemble=ensemble, obs_cell=obs_cell, obs_value=obs_value, obs_var=obs_var, obs_frac=obs_frac, loc_column=loc_column, loc_level=loc_level)


def obs_stats(prior_obs, obs_val, variance):
    members = prior_obs.shape[1]
    obs_mean = lax.optimization_barrier(jnp.mean(prior_obs, axis=1))
    deviation = prior_obs - obs_mean[:, None]
    spread = lax.optimization_barrier(jnp.sum(deviation * deviation, axis=1)) / (members - 1.0)
    total_var = spread + variance
    shrink = 1.0 / (1.0 + jnp.sqrt(variance / total_var))
    gain_rows = ((obs_val - obs_mean)[:, None] - deviation * shrink[:, None]) / (total_var * (members - 1.0))[:, None]
    return (obs_mean, deviation.astype(jnp.bfloat16), gain_rows.astype(jnp.bfloat16))

def reference(ensemble, obs_cell, obs_value, obs_var, obs_frac, loc_column, loc_level):
    current = ensemble
    prior_means = []
    for block_index in range(BLOCKS):
        obs_cells = obs_cell[block_index]
        obs_level = obs_cells // NC
        obs_column = obs_cells % NC
        next_column = (obs_column + 1) % NC
        flattened = current.reshape(MEM, NL * NC)
        first_val = jnp.take(flattened, obs_level * NC + obs_column, axis=1)
        second = jnp.take(flattened, obs_level * NC + next_column, axis=1)
        fraction = obs_frac[block_index]
        prior_obs = ((1.0 - fraction)[None, :] * first_val + fraction[None, :] * second).T
        obs_mean, dev_b, gain_b = obs_stats(prior_obs, obs_value[block_index], obs_var[block_index])
        prior_means.append(obs_mean)
        centred = (current - lax.optimization_barrier(jnp.mean(current, axis=0))).astype(jnp.bfloat16)
        col_weights = loc_column[block_index]
        lev_weights = loc_level[block_index]

        def level_step(level_index):
            level_slab = lax.dynamic_index_in_dim(centred, level_index, 1, keepdims=False)
            level_loc = lax.dynamic_index_in_dim(lev_weights, level_index, 1, keepdims=False)
            cross_cov = jnp.dot(dev_b, level_slab, preferred_element_type=jnp.float32)
            mixed_rows = (level_loc[:, None] * col_weights.astype(jnp.float32) * cross_cov).astype(jnp.bfloat16)
            return jnp.dot(gain_b.T, mixed_rows, preferred_element_type=jnp.float32)
        increment = lax.map(level_step, jnp.arange(NL, dtype=jnp.int32))
        current = current + jnp.transpose(increment, (1, 0, 2))
    return (current, jnp.stack(prior_means))
```

```python
import functools

import jax
import jax.numpy as jnp
from jax import lax
from jax.experimental import pallas as pl
from jax.experimental.pallas import tpu as pltpu
from jax.sharding import PartitionSpec as P

MESH = pl.DeviceIdType.MESH
LANES = 128
F32 = jnp.float32
BF16 = jnp.bfloat16


def pick_kernel(block, members, lev_rows, n_slab, cell_ref, frac_ref, ens_ref, out_ref, acc):
    n_obs = cell_ref.shape[1]
    tiles = ens_ref.shape[0] // (members * lev_rows)
    slab_cols = tiles * LANES
    total = slab_cols * n_slab
    base = lax.axis_index("lev") * (lev_rows * total)
    col_base = lax.axis_index("slab") * slab_cols
    acc[...] = jnp.zeros_like(acc)
    lane_ids = lax.broadcasted_iota(jnp.int32, (members, LANES), 1)

    def body(j, carry):
        rest = cell_ref[block, j] - base
        frac = frac_ref[block, j]
        row = jnp.int32(0)
        for level in range(1, lev_rows):
            row = row + (rest >= level * total).astype(jnp.int32)
        in_band = (rest >= 0) & (rest < lev_rows * total)
        col = rest - row * total
        following = jnp.where(col + 1 == total, 0, col + 1)
        tile_at = lax.shift_right_logical(j, 7)
        lane_at = j & (LANES - 1)

        def add(column, weight):
            local = column - col_base

            @pl.when(in_band & (local >= 0) & (local < slab_cols))
            def _():
                start = lax.shift_right_logical(local, 7) * lev_rows + row
                window = ens_ref[pl.ds(start, members, stride=tiles * lev_rows), :]
                moved = pltpu.roll(window, (lane_at - (local & (LANES - 1))) & (LANES - 1), 1)
                old = acc[tile_at, :members, :]
                acc[tile_at, :members, :] = old + jnp.where(lane_ids == lane_at, moved * weight, 0.0)

        add(col, 1.0 - frac)
        add(following, frac)
        return carry

    lax.fori_loop(0, n_obs, body, 0)
    for t in range(n_obs // LANES):
        out_ref[t * LANES : (t + 1) * LANES, :] = acc[t].T


def pick(block, n_slab, members, lev_rows, cells, fracs, flat):
    n_obs = cells.shape[1]
    return pl.pallas_call(
        functools.partial(pick_kernel, block, members, lev_rows, n_slab),
        out_shape=jax.ShapeDtypeStruct((n_obs, LANES), F32),
        in_specs=[
            pl.BlockSpec(memory_space=pltpu.SMEM),
            pl.BlockSpec(memory_space=pltpu.SMEM),
            pl.BlockSpec(memory_space=pltpu.VMEM),
        ],
        out_specs=pl.BlockSpec(memory_space=pltpu.VMEM),
        scratch_shapes=[pltpu.VMEM((n_obs // LANES, LANES, LANES), F32)],
        name="pick",
    )(cells, fracs, flat)


def exchange_kernel(
    n_slab, n_lev, pieces, part_ref, loc_ref, prior_ref, gat_ref, landed, own,
    scat_send, scat_recv, cast_send, cast_recv, up_send, down_send, line_recv,
):
    n = n_slab * n_lev
    slab, lev = lax.axis_index("slab"), lax.axis_index("lev")
    me = slab * n_lev + lev
    rows = loc_ref.shape[1]
    cut = rows // pieces

    def peer(k):
        p = lax.rem(me + k, n)
        return p, (p // n_lev, lax.rem(p, n_lev))

    barrier = pltpu.get_barrier_semaphore()

    def greet(k, c):
        _, where = peer(k)
        pl.semaphore_signal(barrier, inc=1, device_id=where, device_id_type=MESH)
        return c

    lax.fori_loop(1, n, greet, 0)
    pl.semaphore_wait(barrier, n - 1)

    def scatter(k):
        p, where = peer(k)
        return pltpu.make_async_remote_copy(
            src_ref=part_ref.at[p], dst_ref=landed.at[k], send_sem=scat_send.at[k],
            recv_sem=scat_recv.at[k], device_id=where, device_id_type=MESH)

    def cast(k):
        _, where = peer(k)
        return pltpu.make_async_remote_copy(
            src_ref=own, dst_ref=prior_ref.at[me], send_sem=cast_send.at[k],
            recv_sem=cast_recv.at[k], device_id=where, device_id_type=MESH)

    def each(act):
        def body(k, c):
            act(k)
            return c
        lax.fori_loop(1, n, body, 0)

    def slot(source, h):
        return gat_ref.at[pl.ds(pl.multiple_of(source * rows + h * cut, cut), cut), :]

    def hop(source, h, first, step):
        src = loc_ref.at[0, pl.ds(h * cut, cut), :] if first else slot(source, h)
        sems = up_send if step > 0 else down_send
        return pltpu.make_async_remote_copy(
            src_ref=src, dst_ref=slot(source, h), send_sem=sems.at[source, h],
            recv_sem=line_recv.at[source, h], device_id=(slab, lev + step), device_id_type=MESH)

    each(lambda k: scatter(k).start())
    for h in range(pieces):
        @pl.when(lev < n_lev - 1)
        def _():
            hop(lev, h, True, 1).start()

        @pl.when(lev > 0)
        def _():
            hop(lev, h, True, -1).start()

    gat_ref[pl.ds(pl.multiple_of(lev * rows, rows), rows), :] = loc_ref[0]

    each(lambda k: scatter(k).wait_recv())
    landed[0] = part_ref[me]
    own[...] = jnp.sum(landed[...], axis=0)
    each(lambda k: cast(k).start())
    prior_ref[me] = own[...]

    for s in range(1, n_lev):
        for h in range(pieces):
            @pl.when(lev - s >= 0)
            def _():
                hop(lev - s, h, False, 1).wait_recv()

                @pl.when(lev < n_lev - 1)
                def _():
                    hop(lev - s, h, False, 1).start()

            @pl.when(lev + s <= n_lev - 1)
            def _():
                hop(lev + s, h, False, -1).wait_recv()

                @pl.when(lev > 0)
                def _():
                    hop(lev + s, h, False, -1).start()

    each(lambda k: cast(k).wait_recv())
    each(lambda k: scatter(k).wait_send())
    each(lambda k: cast(k).wait_send())
    for s in range(n_lev):
        for h in range(pieces):
            @pl.when((lev - s >= 0) & (lev < n_lev - 1))
            def _():
                hop(lev - s, h, s == 0, 1).wait_send()

            @pl.when((lev + s <= n_lev - 1) & (lev > 0))
            def _():
                hop(lev + s, h, s == 0, -1).wait_send()


def exchange(block, n_slab, n_lev, part, loc):
    n = n_slab * n_lev
    n_obs = part.shape[0]
    per = n_obs // n
    rows, cols = loc.shape[1:]
    pieces = 2
    prior, gathered = pl.pallas_call(
        functools.partial(exchange_kernel, n_slab, n_lev, pieces),
        grid=(1,),
        out_shape=[
            jax.ShapeDtypeStruct((n, per, LANES), F32),
            jax.ShapeDtypeStruct((n_obs, cols), BF16),
        ],
        in_specs=[
            pl.BlockSpec((n, per, LANES), lambda i: (0, 0, 0)),
            pl.BlockSpec((1, rows, cols), lambda i: (block, 0, 0)),
        ],
        out_specs=[
            pl.BlockSpec((n, per, LANES), lambda i: (0, 0, 0)),
            pl.BlockSpec((n_obs, cols), lambda i: (0, 0)),
        ],
        scratch_shapes=[
            pltpu.VMEM((n, per, LANES), F32),
            pltpu.VMEM((per, LANES), F32),
            pltpu.SemaphoreType.DMA((n,)),
            pltpu.SemaphoreType.DMA((n,)),
            pltpu.SemaphoreType.DMA((n,)),
            pltpu.SemaphoreType.DMA((n,)),
            pltpu.SemaphoreType.DMA((n_lev, pieces)),
            pltpu.SemaphoreType.DMA((n_lev, pieces)),
            pltpu.SemaphoreType.DMA((n_lev, pieces)),
        ],
        compiler_params=pltpu.CompilerParams(collective_id=block, has_side_effects=True),
        name="exchange",
    )(part.reshape(n, per, LANES), loc)
    return prior.reshape(n_obs, LANES), gathered


def update_kernel(block, lev_rows, prior_ref, value_ref, var_ref, lev_ref, loc_ref, ens_ref, out_ref, mean_ref, dev_s, gain_s):
    members = ens_ref.shape[0]
    group = ens_ref.shape[1]
    n_obs = prior_ref.shape[0]

    @pl.when(pl.program_id(0) == 0)
    def _():
        def column(ref):
            return jnp.broadcast_to(ref[block : block + 1, :], (8, n_obs)).T[:, :1]

        value, var = column(value_ref), column(var_ref)
        prior = prior_ref[...]
        live = lax.broadcasted_iota(jnp.int32, prior.shape, 1) < members
        mean = jnp.sum(jnp.where(live, prior, 0.0), axis=1, keepdims=True) / members
        deviation = jnp.where(live, prior - mean, 0.0)
        spread = jnp.sum(deviation * deviation, axis=1, keepdims=True) / (members - 1.0)
        total = spread + var
        shrink = 1.0 / (1.0 + jnp.sqrt(var / total))
        gain = ((value - mean) - deviation * shrink) / (total * (members - 1.0))
        dev_s[...] = deviation.astype(BF16)
        gain_s[...] = gain.T.astype(BF16)
        mean_ref[...] = jnp.broadcast_to(mean, (n_obs, LANES)).T[:8, :]

    dev = dev_s[:, :members]
    gain = gain_s[:members, :]
    rows_in = ens_ref.reshape(members * group, LANES)
    rows_out = out_ref.reshape(members * group, LANES)
    tiles = group // lev_rows
    loc = loc_ref[...].astype(F32)
    for level in range(lev_rows):
        spots = [pl.ds(t * lev_rows + level, members, stride=group) for t in range(tiles)]
        now = jnp.concatenate([rows_in[spot, :] for spot in spots], axis=1)
        centred = (now - jnp.sum(now, axis=0, keepdims=True) / members).astype(BF16)
        cross = jnp.dot(dev, centred, preferred_element_type=F32)
        mixed = ((lev_ref[:, level : level + 1] * loc) * cross).astype(BF16)
        new = now + jnp.dot(gain, mixed, preferred_element_type=F32)
        for t, spot in enumerate(spots):
            rows_out[spot, :] = new[:, t * LANES : (t + 1) * LANES]


def update(block, lev_rows, prior, values, variances, levels, gathered, state):
    members, depth, _ = state.shape
    n_obs = prior.shape[0]
    tiles = 2
    group = tiles * lev_rows
    steps = depth // group
    return pl.pallas_call(
        functools.partial(update_kernel, block, lev_rows),
        grid=(steps,),
        out_shape=[
            jax.ShapeDtypeStruct(state.shape, F32),
            jax.ShapeDtypeStruct((8, n_obs), F32),
        ],
        in_specs=[
            pl.BlockSpec((n_obs, LANES), lambda i: (0, 0)),
            pl.BlockSpec(values.shape, lambda i: (0, 0)),
            pl.BlockSpec(values.shape, lambda i: (0, 0)),
            pl.BlockSpec((None, n_obs, lev_rows), lambda i: (block, 0, 0)),
            pl.BlockSpec((n_obs, tiles * LANES), lambda i: (0, i)),
            pl.BlockSpec((members, group, LANES), lambda i: (0, i, 0)),
        ],
        out_specs=[
            pl.BlockSpec((members, group, LANES), lambda i: (0, i, 0)),
            pl.BlockSpec((8, n_obs), lambda i: (0, 0)),
        ],
        scratch_shapes=[pltpu.VMEM((n_obs, LANES), BF16), pltpu.VMEM((LANES, n_obs), BF16)],
        compiler_params=pltpu.CompilerParams(dimension_semantics=("arbitrary",)),
        name="update",
    )(prior, values, variances, levels, gathered, state)


def solution(mesh):
    n_slab, n_lev = mesh.shape["slab"], mesh.shape["lev"]

    def on_device(ensemble, obs_cell, obs_value, obs_var, obs_frac, loc_column, loc_level):
        members, lev_rows, cols = ensemble.shape
        tiles = cols // LANES
        state = ensemble.reshape(members, lev_rows, tiles, LANES).transpose(0, 2, 1, 3)
        state = state.reshape(members, tiles * lev_rows, LANES)
        means = []
        for block in range(obs_cell.shape[0]):
            flat = state.reshape(members * tiles * lev_rows, LANES)
            part = pick(block, n_slab, members, lev_rows, obs_cell, obs_frac, flat)
            prior, gathered = exchange(block, n_slab, n_lev, part, loc_column)
            state, mean = update(block, lev_rows, prior, obs_value, obs_var, loc_level, gathered, state)
            means.append(mean[0])
        analysis = state.reshape(members, tiles, lev_rows, LANES).transpose(0, 2, 1, 3)
        return analysis.reshape(members, lev_rows, cols), jnp.stack(means)

    in_specs = (
        P(None, "lev", "slab"), P(), P(), P(), P(),
        P(None, "lev", "slab"), P(None, None, "lev"),
    )
    return jax.shard_map(
        on_device, mesh=mesh, in_specs=in_specs,
        out_specs=(P(None, "lev", "slab"), P()), check_vma=False,
    )
```

```python
import functools

import jax
import jax.numpy as jnp
from jax import lax
from jax.experimental import pallas as pl
from jax.experimental.pallas import tpu as pltpu
from jax.sharding import PartitionSpec as P

MESH = pl.DeviceIdType.MESH
LANES = 128
F32 = jnp.float32
BF16 = jnp.bfloat16


def pick_kernel(block, members, lev_rows, n_slab, cell_ref, frac_ref, ens_ref, out_ref, acc, list_ref):
    n_obs = cell_ref.shape[1]
    raw = len(ens_ref.shape) == 3
    tiles = ens_ref.shape[2] // LANES if raw else ens_ref.shape[0] // (members * lev_rows)
    slab_cols = tiles * LANES
    total = slab_cols * n_slab
    base = lax.axis_index("lev") * (lev_rows * total)
    col_base = lax.axis_index("slab") * slab_cols
    acc[...] = jnp.zeros_like(acc)
    lane_ids = lax.broadcasted_iota(jnp.int32, (members, LANES), 1)

    def place(j):
        rest = cell_ref[block, j] - base
        row = jnp.int32(0)
        for level in range(1, lev_rows):
            row = row + (rest >= level * total).astype(jnp.int32)
        col = rest - row * total
        following = jnp.where(col + 1 == total, 0, col + 1)
        first, second = col - col_base, following - col_base
        in_band = (rest >= 0) & (rest < lev_rows * total)
        has_first = in_band & (first >= 0) & (first < slab_cols)
        has_second = in_band & (second >= 0) & (second < slab_cols)
        return row, first, second, has_first, has_second

    def scan(j, count):
        _, _, _, has_first, has_second = place(j)
        list_ref[count] = j
        return count + (has_first | has_second).astype(jnp.int32)

    count = lax.fori_loop(0, n_obs, scan, jnp.int32(0), unroll=8)

    def body(at, carry):
        j = list_ref[at]
        row, first, second, has_first, has_second = place(j)
        frac = frac_ref[block, j]
        tile_at = lax.shift_right_logical(j, 7)
        lane_at = j & (LANES - 1)

        def share(local, weight, mine):
            local = jnp.where(mine, local, 0)
            tile = lax.shift_right_logical(local, 7)
            if raw:
                lanes = pl.ds(pl.multiple_of(tile * LANES, LANES), LANES)
                window = ens_ref[:, 0, lanes]
                for level in range(1, lev_rows):
                    window = jnp.where(row == level, ens_ref[:, level, lanes], window)
            else:
                window = ens_ref[pl.ds(tile * lev_rows + row, members, stride=tiles * lev_rows), :]
            moved = pltpu.roll(window, (lane_at - (local & (LANES - 1))) & (LANES - 1), 1)
            return moved * jnp.where(mine, weight, 0.0)

        value = share(first, 1.0 - frac, has_first) + share(second, frac, has_second)
        old = acc[tile_at, :members, :]
        acc[tile_at, :members, :] = jnp.where(lane_ids == lane_at, value, old)
        return carry

    lax.fori_loop(0, count, body, 0)
    for t in range(n_obs // LANES):
        out_ref[t * LANES : (t + 1) * LANES, :] = acc[t].T


def pick(block, n_slab, members, lev_rows, cells, fracs, flat):
    n_obs = cells.shape[1]
    return pl.pallas_call(
        functools.partial(pick_kernel, block, members, lev_rows, n_slab),
        out_shape=jax.ShapeDtypeStruct((n_obs, LANES), F32),
        in_specs=[
            pl.BlockSpec(memory_space=pltpu.SMEM),
            pl.BlockSpec(memory_space=pltpu.SMEM),
            pl.BlockSpec(memory_space=pltpu.VMEM),
        ],
        out_specs=pl.BlockSpec(memory_space=pltpu.VMEM),
        scratch_shapes=[pltpu.VMEM((n_obs // LANES, LANES, LANES), F32), pltpu.SMEM((n_obs + 1,), jnp.int32)],
        name="pick",
    )(cells, fracs, flat)


def exchange_kernel(
    n_slab, n_lev, pieces, part_ref, loc_ref, prior_ref, gat_ref, landed, own,
    scat_send, scat_recv, cast_send, cast_recv, up_send, down_send, line_recv,
):
    n = n_slab * n_lev
    slab, lev = lax.axis_index("slab"), lax.axis_index("lev")
    me = slab * n_lev + lev
    rows = loc_ref.shape[1]
    cut = rows // pieces

    def peer(k):
        p = lax.rem(me + k, n)
        return p, (p // n_lev, lax.rem(p, n_lev))

    barrier = pltpu.get_barrier_semaphore()

    def greet(k, c):
        _, where = peer(k)
        pl.semaphore_signal(barrier, inc=1, device_id=where, device_id_type=MESH)
        return c

    lax.fori_loop(1, n, greet, 0)
    pl.semaphore_wait(barrier, n - 1)

    def scatter(k):
        p, where = peer(k)
        return pltpu.make_async_remote_copy(
            src_ref=part_ref.at[p], dst_ref=landed.at[k], send_sem=scat_send.at[k],
            recv_sem=scat_recv.at[k], device_id=where, device_id_type=MESH)

    def cast(k):
        _, where = peer(k)
        return pltpu.make_async_remote_copy(
            src_ref=own, dst_ref=prior_ref.at[me], send_sem=cast_send.at[k],
            recv_sem=cast_recv.at[k], device_id=where, device_id_type=MESH)

    def each(act):
        def body(k, c):
            act(k)
            return c
        lax.fori_loop(1, n, body, 0)

    def slot(source, h):
        return gat_ref.at[pl.ds(pl.multiple_of(source * rows + h * cut, cut), cut), :]

    def hop(source, h, first, step):
        src = loc_ref.at[0, pl.ds(h * cut, cut), :] if first else slot(source, h)
        sems = up_send if step > 0 else down_send
        return pltpu.make_async_remote_copy(
            src_ref=src, dst_ref=slot(source, h), send_sem=sems.at[source, h],
            recv_sem=line_recv.at[source, h], device_id=(slab, lev + step), device_id_type=MESH)

    each(lambda k: scatter(k).start())
    for h in range(pieces):
        @pl.when(lev < n_lev - 1)
        def _():
            hop(lev, h, True, 1).start()

        @pl.when(lev > 0)
        def _():
            hop(lev, h, True, -1).start()

    gat_ref[pl.ds(pl.multiple_of(lev * rows, rows), rows), :] = loc_ref[0]

    each(lambda k: scatter(k).wait_recv())
    landed[0] = part_ref[me]
    own[...] = jnp.sum(landed[...], axis=0)
    each(lambda k: cast(k).start())
    prior_ref[me] = own[...]

    for s in range(1, n_lev):
        for h in range(pieces):
            @pl.when(lev - s >= 0)
            def _():
                hop(lev - s, h, False, 1).wait_recv()

                @pl.when(lev < n_lev - 1)
                def _():
                    hop(lev - s, h, False, 1).start()

            @pl.when(lev + s <= n_lev - 1)
            def _():
                hop(lev + s, h, False, -1).wait_recv()

                @pl.when(lev > 0)
                def _():
                    hop(lev + s, h, False, -1).start()

    each(lambda k: cast(k).wait_recv())
    each(lambda k: scatter(k).wait_send())
    each(lambda k: cast(k).wait_send())
    for s in range(n_lev):
        for h in range(pieces):
            @pl.when((lev - s >= 0) & (lev < n_lev - 1))
            def _():
                hop(lev - s, h, s == 0, 1).wait_send()

            @pl.when((lev + s <= n_lev - 1) & (lev > 0))
            def _():
                hop(lev + s, h, s == 0, -1).wait_send()


def exchange(block, n_slab, n_lev, part, loc):
    n = n_slab * n_lev
    n_obs = part.shape[0]
    per = n_obs // n
    rows, cols = loc.shape[1:]
    pieces = 2
    prior, gathered = pl.pallas_call(
        functools.partial(exchange_kernel, n_slab, n_lev, pieces),
        grid=(1,),
        out_shape=[
            jax.ShapeDtypeStruct((n, per, LANES), F32),
            jax.ShapeDtypeStruct((n_obs, cols), BF16),
        ],
        in_specs=[
            pl.BlockSpec((n, per, LANES), lambda i: (0, 0, 0)),
            pl.BlockSpec((1, rows, cols), lambda i: (block, 0, 0)),
        ],
        out_specs=[
            pl.BlockSpec((n, per, LANES), lambda i: (0, 0, 0)),
            pl.BlockSpec((n_obs, cols), lambda i: (0, 0)),
        ],
        scratch_shapes=[
            pltpu.VMEM((n, per, LANES), F32),
            pltpu.VMEM((per, LANES), F32),
            pltpu.SemaphoreType.DMA((n,)),
            pltpu.SemaphoreType.DMA((n,)),
            pltpu.SemaphoreType.DMA((n,)),
            pltpu.SemaphoreType.DMA((n,)),
            pltpu.SemaphoreType.DMA((n_lev, pieces)),
            pltpu.SemaphoreType.DMA((n_lev, pieces)),
            pltpu.SemaphoreType.DMA((n_lev, pieces)),
        ],
        compiler_params=pltpu.CompilerParams(collective_id=block, has_side_effects=True),
        name="exchange",
    )(part.reshape(n, per, LANES), loc)
    return prior.reshape(n_obs, LANES), gathered


def update_kernel(block, lev_rows, raw_in, raw_out, prior_ref, value_ref, var_ref, lev_ref, old_ref, loc_ref, ens_ref, out_ref, mean_ref, dev_s, gain_s, lev_s):
    members = ens_ref.shape[0]
    n_obs = prior_ref.shape[0]
    tiles = loc_ref.shape[1] // LANES
    group = tiles * lev_rows

    @pl.when(pl.program_id(0) == 0)
    def _():
        def column(ref):
            return jnp.broadcast_to(ref[block : block + 1, :], (8, n_obs)).T[:, :1]

        value, var = column(value_ref), column(var_ref)
        prior = prior_ref[...]
        live = lax.broadcasted_iota(jnp.int32, prior.shape, 1) < members
        mean = jnp.sum(jnp.where(live, prior, 0.0), axis=1, keepdims=True) / members
        deviation = jnp.where(live, prior - mean, 0.0)
        spread = jnp.sum(deviation * deviation, axis=1, keepdims=True) / (members - 1.0)
        total = spread + var
        shrink = 1.0 / (1.0 + jnp.sqrt(var / total))
        gain = ((value - mean) - deviation * shrink) / (total * (members - 1.0))
        dev_s[...] = deviation.astype(BF16)
        gain_s[...] = gain.T.astype(BF16)
        mean_ref[...] = old_ref[...]
        mean_ref[block : block + 1, :] = jnp.broadcast_to(mean, (n_obs, LANES)).T[:1, :]
        for level in range(lev_rows):
            lev_s[level] = jnp.broadcast_to(lev_ref[level : level + 1, :], (LANES, n_obs)).T

    dev = dev_s[:, :members]
    gain = gain_s[:members, :]
    rows_in = None if raw_in else ens_ref.reshape(members * group, LANES)
    rows_out = None if raw_out else out_ref.reshape(members * group, LANES)
    loc = loc_ref[...].astype(F32)
    for level in range(lev_rows):
        spots = [pl.ds(t * lev_rows + level, members, stride=group) for t in range(tiles)]
        if raw_in:
            now = ens_ref[:, level, :]
        else:
            now = jnp.concatenate([rows_in[spot, :] for spot in spots], axis=1)
        centred = (now - jnp.sum(now, axis=0, keepdims=True) / members).astype(BF16)
        cross = jnp.dot(dev, centred, preferred_element_type=F32)
        height = jnp.concatenate([lev_s[level]] * tiles, axis=1)
        mixed = ((height * loc) * cross).astype(BF16)
        new = now + jnp.dot(gain, mixed, preferred_element_type=F32)
        if raw_out:
            out_ref[:, level, :] = new
        else:
            for t, spot in enumerate(spots):
                rows_out[spot, :] = new[:, t * LANES : (t + 1) * LANES]


def update(block, n_blocks, lev_rows, prior, values, variances, levels, olds, gathered, state):
    members = state.shape[0]
    n_obs = prior.shape[0]
    tiles = next(t for t in (6, 4, 2) if gathered.shape[1] % (t * LANES) == 0)
    group = tiles * lev_rows
    cols = gathered.shape[1]
    steps = cols // (tiles * LANES)
    raw_in, raw_out = block == 0, block == n_blocks - 1
    raw_spec = pl.BlockSpec((members, lev_rows, tiles * LANES), lambda i: (0, 0, i))
    row_spec = pl.BlockSpec((members, group, LANES), lambda i: (0, i, 0))
    out_dims = (members, lev_rows, cols) if raw_out else (members, steps * group, LANES)
    return pl.pallas_call(
        functools.partial(update_kernel, block, lev_rows, raw_in, raw_out),
        grid=(steps,),
        out_shape=[
            jax.ShapeDtypeStruct(out_dims, F32),
            jax.ShapeDtypeStruct(values.shape, F32),
        ],
        in_specs=[
            pl.BlockSpec((n_obs, LANES), lambda i: (0, 0)),
            pl.BlockSpec(values.shape, lambda i: (0, 0)),
            pl.BlockSpec(values.shape, lambda i: (0, 0)),
            pl.BlockSpec((None, lev_rows, n_obs), lambda i: (block, 0, 0)),
            pl.BlockSpec(olds.shape, lambda i: (0, 0)),
            pl.BlockSpec((n_obs, tiles * LANES), lambda i: (0, i)),
            raw_spec if raw_in else row_spec,
        ],
        out_specs=[
            raw_spec if raw_out else row_spec,
            pl.BlockSpec(values.shape, lambda i: (0, 0)),
        ],
        scratch_shapes=[pltpu.VMEM((n_obs, LANES), BF16), pltpu.VMEM((LANES, n_obs), BF16), pltpu.VMEM((lev_rows, n_obs, LANES), F32)],
        compiler_params=pltpu.CompilerParams(dimension_semantics=("arbitrary",)),
        name="update",
    )(prior, values, variances, levels, olds, gathered, state)


def solution(mesh):
    n_slab, n_lev = mesh.shape["slab"], mesh.shape["lev"]

    def on_device(ensemble, obs_cell, obs_value, obs_var, obs_frac, loc_column, loc_level):
        members, lev_rows, cols = ensemble.shape
        n_blocks = obs_cell.shape[0]
        state = ensemble
        means, heights = obs_value, loc_level.transpose(0, 2, 1)
        for block in range(n_blocks):
            flat = state if block == 0 else state.reshape(members * cols // LANES * lev_rows, LANES)
            part = pick(block, n_slab, members, lev_rows, obs_cell, obs_frac, flat)
            prior, gathered = exchange(block, n_slab, n_lev, part, loc_column)
            state, means = update(block, n_blocks, lev_rows, prior, obs_value, obs_var, heights, means, gathered, state)
        return state, means

    in_specs = (
        P(None, "lev", "slab"), P(), P(), P(), P(),
        P(None, "lev", "slab"), P(None, None, "lev"),
    )
    return jax.shard_map(
        on_device, mesh=mesh, in_specs=in_specs,
        out_specs=(P(None, "lev", "slab"), P()), check_vma=False,
    )
```

```python
import functools

import jax
import jax.numpy as jnp
from jax import lax
from jax.experimental import pallas as pl
from jax.experimental.pallas import tpu as pltpu
from jax.sharding import PartitionSpec as P

MESH = pl.DeviceIdType.MESH
LANES = 128
F32 = jnp.float32
BF16 = jnp.bfloat16
COST = pl.CostEstimate(flops=0, bytes_accessed=40_000_000, transcendentals=0)


def pick_kernel(block, members, lev_rows, n_slab, cell_ref, frac_ref, ens_ref, out_ref, acc, list_ref):
    n_obs = cell_ref.shape[1]
    raw = len(ens_ref.shape) == 3
    tiles = ens_ref.shape[2] // LANES if raw else ens_ref.shape[0] // (members * lev_rows)
    slab_cols = tiles * LANES
    total = slab_cols * n_slab
    base = lax.axis_index("lev") * (lev_rows * total)
    col_base = lax.axis_index("slab") * slab_cols
    acc[...] = jnp.zeros_like(acc)
    lane_ids = lax.broadcasted_iota(jnp.int32, (members, LANES), 1)

    def place(j):
        rest = cell_ref[block, j] - base
        row = jnp.int32(0)
        for level in range(1, lev_rows):
            row = row + (rest >= level * total).astype(jnp.int32)
        col = rest - row * total
        following = jnp.where(col + 1 == total, 0, col + 1)
        first, second = col - col_base, following - col_base
        in_band = (rest >= 0) & (rest < lev_rows * total)
        has_first = in_band & (first >= 0) & (first < slab_cols)
        has_second = in_band & (second >= 0) & (second < slab_cols)
        return row, first, second, has_first, has_second

    def scan(j, count):
        _, _, _, has_first, has_second = place(j)
        list_ref[count] = j
        return count + (has_first | has_second).astype(jnp.int32)

    count = lax.fori_loop(0, n_obs, scan, jnp.int32(0), unroll=8)

    def body(at, carry):
        j = list_ref[at]
        row, first, second, has_first, has_second = place(j)
        frac = frac_ref[block, j]
        tile_at = lax.shift_right_logical(j, 7)
        lane_at = j & (LANES - 1)

        def share(local, weight, mine, level):
            local = jnp.where(mine, local, 0)
            tile = lax.shift_right_logical(local, 7)
            if raw:
                window = ens_ref[:, level, pl.ds(pl.multiple_of(tile * LANES, LANES), LANES)]
            else:
                window = ens_ref[pl.ds(tile * lev_rows + row, members, stride=tiles * lev_rows), :]
            moved = pltpu.roll(window, (lane_at - (local & (LANES - 1))) & (LANES - 1), 1)
            return moved * jnp.where(mine, weight, 0.0)

        def put(level):
            value = share(first, 1.0 - frac, has_first, level) + share(second, frac, has_second, level)
            old = acc[tile_at, :members, :]
            acc[tile_at, :members, :] = jnp.where(lane_ids == lane_at, value, old)

        if raw:
            for level in range(lev_rows):
                pl.when(row == level)(functools.partial(put, level))
        else:
            put(0)
        return carry

    lax.fori_loop(0, count, body, 0)
    for t in range(n_obs // LANES):
        out_ref[t * LANES : (t + 1) * LANES, :] = acc[t].T


def pick(block, n_slab, members, lev_rows, cells, fracs, flat):
    n_obs = cells.shape[1]
    return pl.pallas_call(
        functools.partial(pick_kernel, block, members, lev_rows, n_slab),
        out_shape=jax.ShapeDtypeStruct((n_obs, LANES), F32),
        in_specs=[
            pl.BlockSpec(memory_space=pltpu.SMEM),
            pl.BlockSpec(memory_space=pltpu.SMEM),
            pl.BlockSpec(memory_space=pltpu.VMEM),
        ],
        out_specs=pl.BlockSpec(memory_space=pltpu.VMEM),
        scratch_shapes=[pltpu.VMEM((n_obs // LANES, LANES, LANES), F32), pltpu.SMEM((n_obs + 1,), jnp.int32)],
        cost_estimate=COST,
        name="pick",
    )(cells, fracs, flat)


def exchange_kernel(n_slab, n_lev, part_ref, prior_ref, landed, own, scat_send, scat_recv, cast_send, cast_recv):
    n = n_slab * n_lev
    me = lax.axis_index("slab") * n_lev + lax.axis_index("lev")

    def peer(k):
        p = lax.rem(me + k, n)
        return p, (p // n_lev, lax.rem(p, n_lev))

    def each(act):
        def body(k, c):
            act(k)
            return c
        lax.fori_loop(1, n, body, 0)

    barrier = pltpu.get_barrier_semaphore()
    each(lambda k: pl.semaphore_signal(barrier, inc=1, device_id=peer(k)[1], device_id_type=MESH))
    pl.semaphore_wait(barrier, n - 1)

    def scatter(k):
        p, where = peer(k)
        return pltpu.make_async_remote_copy(
            src_ref=part_ref.at[p], dst_ref=landed.at[k], send_sem=scat_send.at[k],
            recv_sem=scat_recv.at[k], device_id=where, device_id_type=MESH)

    def cast(k):
        return pltpu.make_async_remote_copy(
            src_ref=own, dst_ref=prior_ref.at[me], send_sem=cast_send.at[k],
            recv_sem=cast_recv.at[k], device_id=peer(k)[1], device_id_type=MESH)

    each(lambda k: scatter(k).start())
    landed[0] = part_ref[me]
    each(lambda k: scatter(k).wait_recv())
    own[...] = jnp.sum(landed[...], axis=0)
    each(lambda k: cast(k).start())
    prior_ref[me] = own[...]
    each(lambda k: scatter(k).wait_send())
    each(lambda k: cast(k).wait_recv())
    each(lambda k: cast(k).wait_send())


def exchange(block, n_slab, n_lev, part):
    n = n_slab * n_lev
    n_obs = part.shape[0]
    per = n_obs // n
    prior = pl.pallas_call(
        functools.partial(exchange_kernel, n_slab, n_lev),
        out_shape=jax.ShapeDtypeStruct((n, per, LANES), F32),
        in_specs=[pl.BlockSpec(memory_space=pltpu.VMEM)],
        out_specs=pl.BlockSpec(memory_space=pltpu.VMEM),
        scratch_shapes=[
            pltpu.VMEM((n, per, LANES), F32),
            pltpu.VMEM((per, LANES), F32),
            pltpu.SemaphoreType.DMA((n,)),
            pltpu.SemaphoreType.DMA((n,)),
            pltpu.SemaphoreType.DMA((n,)),
            pltpu.SemaphoreType.DMA((n,)),
        ],
        compiler_params=pltpu.CompilerParams(collective_id=block, has_side_effects=True),
        cost_estimate=COST,
        name="exchange",
    )(part.reshape(n, per, LANES))
    return prior.reshape(n_obs, LANES)


def shift(x, n_lev, step):
    pairs = [(i, i + step) for i in range(n_lev) if 0 <= i + step < n_lev]
    return lax.ppermute(x, "lev", pairs)


def update_kernel(
    block, n_lev, lev_rows, raw_in, raw_out, prior_ref, value_ref, var_ref, lev_ref, old_ref, ens_ref, own_ref, *rest
):
    *piece_refs, out_ref, mean_ref, dev_s, gain_s, lev_s, loc_ref = rest
    members = ens_ref.shape[0]
    n_obs = prior_ref.shape[0]
    rows = own_ref.shape[1]
    tiles = loc_ref.shape[1] // LANES
    group = tiles * lev_rows

    @pl.when(pl.program_id(0) == 0)
    def _():
        def column(ref):
            return jnp.broadcast_to(ref[block : block + 1, :], (8, n_obs)).T[:, :1]

        value, var = column(value_ref), column(var_ref)
        prior = prior_ref[...]
        live = lax.broadcasted_iota(jnp.int32, prior.shape, 1) < members
        mean = jnp.sum(jnp.where(live, prior, 0.0), axis=1, keepdims=True) / members
        deviation = jnp.where(live, prior - mean, 0.0)
        spread = jnp.sum(deviation * deviation, axis=1, keepdims=True) / (members - 1.0)
        total = spread + var
        shrink = 1.0 / (1.0 + jnp.sqrt(var / total))
        gain = ((value - mean) - deviation * shrink) / (total * (members - 1.0))
        dev_s[...] = deviation.astype(BF16)
        gain_s[...] = gain.T.astype(BF16)
        mean_ref[...] = old_ref[...]
        mean_ref[block : block + 1, :] = jnp.broadcast_to(mean, (n_obs, LANES)).T[:1, :]
        for level in range(lev_rows):
            lev_s[level] = jnp.broadcast_to(lev_ref[level : level + 1, :], (LANES, n_obs)).T

    dev = dev_s[:, :members]
    gain = gain_s[:members, :]
    rows_in = None if raw_in else ens_ref.reshape(members * group, LANES)
    rows_out = None if raw_out else out_ref.reshape(members * group, LANES)
    lev = lax.axis_index("lev")
    loc_ref[pl.ds(pl.multiple_of(lev * rows, rows), rows), :] = own_ref[0]
    for step in range(1, n_lev):
        for sign in (1, -1):
            source = lev - sign * step
            piece = piece_refs[2 * (step - 1) + (sign < 0)]

            @pl.when((source >= 0) & (source < n_lev))
            def _():
                loc_ref[pl.ds(pl.multiple_of(source * rows, rows), rows), :] = piece[...]

    loc = loc_ref[...].astype(F32)
    for level in range(lev_rows):
        spots = [pl.ds(t * lev_rows + level, members, stride=group) for t in range(tiles)]
        if raw_in:
            now = ens_ref[:, level, :]
        else:
            now = jnp.concatenate([rows_in[spot, :] for spot in spots], axis=1)
        centred = (now - jnp.sum(now, axis=0, keepdims=True) / members).astype(BF16)
        cross = jnp.dot(dev, centred, preferred_element_type=F32)
        height = jnp.concatenate([lev_s[level]] * tiles, axis=1)
        mixed = ((height * loc) * cross).astype(BF16)
        new = now + jnp.dot(gain, mixed, preferred_element_type=F32)
        if raw_out:
            out_ref[:, level, :] = new
        else:
            for t, spot in enumerate(spots):
                rows_out[spot, :] = new[:, t * LANES : (t + 1) * LANES]


def update(block, n_blocks, n_lev, lev_rows, prior, values, variances, levels, olds, state, loc, pieces):
    members = state.shape[0]
    n_obs = prior.shape[0]
    tiles = next(t for t in (6, 4, 2) if loc.shape[2] % (t * LANES) == 0)
    group = tiles * lev_rows
    cols, rows = loc.shape[2], loc.shape[1]
    steps = cols // (tiles * LANES)
    raw_in, raw_out = block == 0, block == n_blocks - 1
    raw_spec = pl.BlockSpec((members, lev_rows, tiles * LANES), lambda i: (0, 0, i))
    row_spec = pl.BlockSpec((members, group, LANES), lambda i: (0, i, 0))
    out_dims = (members, lev_rows, cols) if raw_out else (members, steps * group, LANES)
    return pl.pallas_call(
        functools.partial(update_kernel, block, n_lev, lev_rows, raw_in, raw_out),
        grid=(steps,),
        out_shape=[
            jax.ShapeDtypeStruct(out_dims, F32),
            jax.ShapeDtypeStruct(values.shape, F32),
        ],
        in_specs=[
            pl.BlockSpec((n_obs, LANES), lambda i: (0, 0)),
            pl.BlockSpec(values.shape, lambda i: (0, 0)),
            pl.BlockSpec(values.shape, lambda i: (0, 0)),
            pl.BlockSpec((None, lev_rows, n_obs), lambda i: (block, 0, 0)),
            pl.BlockSpec(olds.shape, lambda i: (0, 0)),
            raw_spec if raw_in else row_spec,
            pl.BlockSpec((1, rows, tiles * LANES), lambda i: (block, 0, i)),
        ] + [pl.BlockSpec((rows, tiles * LANES), lambda i: (0, i))] * len(pieces) + [
        ],
        out_specs=[
            raw_spec if raw_out else row_spec,
            pl.BlockSpec(values.shape, lambda i: (0, 0)),
        ],
        scratch_shapes=[pltpu.VMEM((n_obs, LANES), BF16), pltpu.VMEM((LANES, n_obs), BF16), pltpu.VMEM((lev_rows, n_obs, LANES), F32), pltpu.VMEM((n_obs, tiles * LANES), BF16)],
        compiler_params=pltpu.CompilerParams(dimension_semantics=("arbitrary",)),
        cost_estimate=COST,
        name="update",
    )(prior, values, variances, levels, olds, state, loc, *pieces)


def solution(mesh):
    n_slab, n_lev = mesh.shape["slab"], mesh.shape["lev"]

    def on_device(ensemble, obs_cell, obs_value, obs_var, obs_frac, loc_column, loc_level):
        members, lev_rows, cols = ensemble.shape
        n_blocks = obs_cell.shape[0]
        state = ensemble
        means, heights = obs_value, loc_level.transpose(0, 2, 1)
        near = [(shift(loc_column[b], n_lev, 1), shift(loc_column[b], n_lev, -1)) for b in range(n_blocks)]
        far = [None] * n_blocks

        def send_on(b):
            far[b] = [shift(near[b][way], n_lev, sign * step) for step in range(1, n_lev - 1) for way, sign in enumerate((1, -1))]

        for block in range(n_blocks):
            flat = state if block == 0 else state.reshape(members * cols // LANES * lev_rows, LANES)
            part = pick(block, n_slab, members, lev_rows, obs_cell, obs_frac, flat)
            if block == 0:
                part, near[0] = lax.optimization_barrier((part, near[0]))
                send_on(0)
            prior = exchange(block, n_slab, n_lev, part)
            if block + 1 < n_blocks:
                prior, near[block + 1] = lax.optimization_barrier((prior, near[block + 1]))
                send_on(block + 1)
            pieces = [*near[block], *far[block]]
            state, means = update(
                block, n_blocks, n_lev, lev_rows, prior, obs_value, obs_var, heights, means, state, loc_column, pieces)
        return state, means

    in_specs = (
        P(None, "lev", "slab"), P(), P(), P(), P(),
        P(None, "lev", "slab"), P(None, None, "lev"),
    )
    return jax.shard_map(
        on_device, mesh=mesh, in_specs=in_specs,
        out_specs=(P(None, "lev", "slab"), P()), check_vma=False,
    )
```

```python
import functools

import jax
import jax.numpy as jnp
from jax import lax
from jax.experimental import pallas as pl
from jax.experimental.pallas import tpu as pltpu
from jax.sharding import PartitionSpec as P

MESH = pl.DeviceIdType.MESH
LANES = 128
F32 = jnp.float32
BF16 = jnp.bfloat16


def pick_kernel(block, members, lev_rows, n_slab, cell_ref, frac_ref, ens_ref, out_ref, acc, list_ref):
    n_obs = cell_ref.shape[1]
    raw = len(ens_ref.shape) == 3
    tiles = ens_ref.shape[2] // LANES if raw else ens_ref.shape[0] // (members * lev_rows)
    slab_cols = tiles * LANES
    total = slab_cols * n_slab
    base = lax.axis_index("lev") * (lev_rows * total)
    col_base = lax.axis_index("slab") * slab_cols
    acc[...] = jnp.zeros_like(acc)
    lane_ids = lax.broadcasted_iota(jnp.int32, (members, LANES), 1)

    def place(j):
        rest = cell_ref[block, j] - base
        row = jnp.int32(0)
        for level in range(1, lev_rows):
            row = row + (rest >= level * total).astype(jnp.int32)
        col = rest - row * total
        following = jnp.where(col + 1 == total, 0, col + 1)
        first, second = col - col_base, following - col_base
        in_band = (rest >= 0) & (rest < lev_rows * total)
        has_first = in_band & (first >= 0) & (first < slab_cols)
        has_second = in_band & (second >= 0) & (second < slab_cols)
        return row, first, second, has_first, has_second

    def scan(j, count):
        _, _, _, has_first, has_second = place(j)
        list_ref[count] = j
        return count + (has_first | has_second).astype(jnp.int32)

    count = lax.fori_loop(0, n_obs, scan, jnp.int32(0), unroll=8)

    def body(at, carry):
        j = list_ref[at]
        row, first, second, has_first, has_second = place(j)
        frac = frac_ref[block, j]
        tile_at = lax.shift_right_logical(j, 7)
        lane_at = j & (LANES - 1)

        def share(local, weight, mine, level):
            local = jnp.where(mine, local, 0)
            tile = lax.shift_right_logical(local, 7)
            if raw:
                window = ens_ref[:, level, pl.ds(pl.multiple_of(tile * LANES, LANES), LANES)]
            else:
                window = ens_ref[pl.ds(tile * lev_rows + row, members, stride=tiles * lev_rows), :]
            moved = pltpu.roll(window, (lane_at - (local & (LANES - 1))) & (LANES - 1), 1)
            return moved * jnp.where(mine, weight, 0.0)

        def put(level):
            value = share(first, 1.0 - frac, has_first, level) + share(second, frac, has_second, level)
            old = acc[tile_at, :members, :]
            acc[tile_at, :members, :] = jnp.where(lane_ids == lane_at, value, old)

        if raw:
            for level in range(lev_rows):
                pl.when(row == level)(functools.partial(put, level))
        else:
            put(0)
        return carry

    lax.fori_loop(0, count, body, 0)
    for t in range(n_obs // LANES):
        out_ref[t * LANES : (t + 1) * LANES, :] = acc[t].T


def pick(block, n_slab, members, lev_rows, cells, fracs, flat):
    n_obs = cells.shape[1]
    return pl.pallas_call(
        functools.partial(pick_kernel, block, members, lev_rows, n_slab),
        out_shape=jax.ShapeDtypeStruct((n_obs, LANES), F32),
        in_specs=[
            pl.BlockSpec(memory_space=pltpu.SMEM),
            pl.BlockSpec(memory_space=pltpu.SMEM),
            pl.BlockSpec(memory_space=pltpu.VMEM),
        ],
        out_specs=pl.BlockSpec(memory_space=pltpu.VMEM),
        scratch_shapes=[pltpu.VMEM((n_obs // LANES, LANES, LANES), F32), pltpu.SMEM((n_obs + 1,), jnp.int32)],
        name="pick",
    )(cells, fracs, flat)


def exchange_kernel(
    n_slab, n_lev, pieces, part_ref, loc_ref, prior_ref, gat_ref, landed, own,
    scat_send, scat_recv, cast_send, cast_recv, up_send, down_send, line_recv,
):
    n = n_slab * n_lev
    slab, lev = lax.axis_index("slab"), lax.axis_index("lev")
    me = slab * n_lev + lev
    rows = loc_ref.shape[1]
    cut = rows // pieces

    def peer(k):
        p = lax.rem(me + k, n)
        return p, (p // n_lev, lax.rem(p, n_lev))

    barrier = pltpu.get_barrier_semaphore()

    def greet(k, c):
        _, where = peer(k)
        pl.semaphore_signal(barrier, inc=1, device_id=where, device_id_type=MESH)
        return c

    lax.fori_loop(1, n, greet, 0)
    pl.semaphore_wait(barrier, n - 1)

    def scatter(k):
        p, where = peer(k)
        return pltpu.make_async_remote_copy(
            src_ref=part_ref.at[p], dst_ref=landed.at[k], send_sem=scat_send.at[k],
            recv_sem=scat_recv.at[k], device_id=where, device_id_type=MESH)

    def cast(k):
        _, where = peer(k)
        return pltpu.make_async_remote_copy(
            src_ref=own, dst_ref=prior_ref.at[me], send_sem=cast_send.at[k],
            recv_sem=cast_recv.at[k], device_id=where, device_id_type=MESH)

    def each(act):
        def body(k, c):
            act(k)
            return c
        lax.fori_loop(1, n, body, 0)

    def slot(source, h):
        return gat_ref.at[pl.ds(pl.multiple_of(source * rows + h * cut, cut), cut), :]

    def up_hops(h):
        return n_lev // 2 - (n_lev % 2 == 0 and h >= pieces // 2)

    def hops(h, step):
        return up_hops(h) if step > 0 else n_lev - 1 - up_hops(h)

    def back(s):
        return lax.rem(lev + s + n_lev, n_lev)

    def hop(source, h, first, step):
        src = loc_ref.at[0, pl.ds(h * cut, cut), :] if first else slot(source, h)
        sems = up_send if step > 0 else down_send
        return pltpu.make_async_remote_copy(
            src_ref=src, dst_ref=slot(source, h), send_sem=sems.at[source, h],
            recv_sem=line_recv.at[source, h], device_id=(slab, back(step)), device_id_type=MESH)

    each(lambda k: scatter(k).start())
    for h in range(pieces):
        for step in (1, -1):
            if hops(h, step) > 0:
                hop(lev, h, True, step).start()

    gat_ref[pl.ds(pl.multiple_of(lev * rows, rows), rows), :] = loc_ref[0]

    each(lambda k: scatter(k).wait_recv())
    landed[0] = part_ref[me]
    own[...] = jnp.sum(landed[...], axis=0)
    each(lambda k: cast(k).start())
    prior_ref[me] = own[...]

    route = [(s, h, step) for s in range(n_lev) for h in range(pieces) for step in (1, -1)]
    for s, h, step in route:
        if 1 <= s <= hops(h, step):
            hop(back(-s * step), h, False, step).wait_recv()
            if s < hops(h, step):
                hop(back(-s * step), h, False, step).start()

    each(lambda k: cast(k).wait_recv())
    each(lambda k: scatter(k).wait_send())
    each(lambda k: cast(k).wait_send())
    for s, h, step in route:
        if s < hops(h, step):
            hop(back(-s * step), h, s == 0, step).wait_send()


def exchange(block, n_slab, n_lev, part, loc):
    n = n_slab * n_lev
    n_obs = part.shape[0]
    per = n_obs // n
    rows, cols = loc.shape[1:]
    pieces = 2
    prior, gathered = pl.pallas_call(
        functools.partial(exchange_kernel, n_slab, n_lev, pieces),
        grid=(1,),
        out_shape=[
            jax.ShapeDtypeStruct((n, per, LANES), F32),
            jax.ShapeDtypeStruct((n_obs, cols), BF16),
        ],
        in_specs=[
            pl.BlockSpec((n, per, LANES), lambda i: (0, 0, 0)),
            pl.BlockSpec((1, rows, cols), lambda i: (block, 0, 0)),
        ],
        out_specs=[
            pl.BlockSpec((n, per, LANES), lambda i: (0, 0, 0)),
            pl.BlockSpec((n_obs, cols), lambda i: (0, 0)),
        ],
        scratch_shapes=[
            pltpu.VMEM((n, per, LANES), F32),
            pltpu.VMEM((per, LANES), F32),
            pltpu.SemaphoreType.DMA((n,)),
            pltpu.SemaphoreType.DMA((n,)),
            pltpu.SemaphoreType.DMA((n,)),
            pltpu.SemaphoreType.DMA((n,)),
            pltpu.SemaphoreType.DMA((n_lev, pieces)),
            pltpu.SemaphoreType.DMA((n_lev, pieces)),
            pltpu.SemaphoreType.DMA((n_lev, pieces)),
        ],
        compiler_params=pltpu.CompilerParams(collective_id=block, has_side_effects=True),
        name="exchange",
    )(part.reshape(n, per, LANES), loc)
    return prior.reshape(n_obs, LANES), gathered


def update_kernel(block, lev_rows, raw_in, raw_out, prior_ref, value_ref, var_ref, lev_ref, old_ref, loc_ref, ens_ref, out_ref, mean_ref, dev_s, gain_s, lev_s):
    members = ens_ref.shape[0]
    n_obs = prior_ref.shape[0]
    tiles = loc_ref.shape[1] // LANES
    group = tiles * lev_rows

    @pl.when(pl.program_id(0) == 0)
    def _():
        def column(ref):
            return jnp.broadcast_to(ref[block : block + 1, :], (8, n_obs)).T[:, :1]

        value, var = column(value_ref), column(var_ref)
        prior = prior_ref[...]
        live = lax.broadcasted_iota(jnp.int32, prior.shape, 1) < members
        mean = jnp.sum(jnp.where(live, prior, 0.0), axis=1, keepdims=True) / members
        deviation = jnp.where(live, prior - mean, 0.0)
        spread = jnp.sum(deviation * deviation, axis=1, keepdims=True) / (members - 1.0)
        total = spread + var
        shrink = 1.0 / (1.0 + jnp.sqrt(var / total))
        gain = ((value - mean) - deviation * shrink) / (total * (members - 1.0))
        dev_s[...] = deviation.astype(BF16)
        gain_s[...] = gain.T.astype(BF16)
        mean_ref[...] = old_ref[...]
        mean_ref[block : block + 1, :] = jnp.broadcast_to(mean, (n_obs, LANES)).T[:1, :]
        for level in range(lev_rows):
            lev_s[level] = jnp.broadcast_to(lev_ref[level : level + 1, :], (LANES, n_obs)).T

    dev = dev_s[:, :members]
    gain = gain_s[:members, :]
    rows_in = None if raw_in else ens_ref.reshape(members * group, LANES)
    rows_out = None if raw_out else out_ref.reshape(members * group, LANES)
    loc = loc_ref[...].astype(F32)
    for level in range(lev_rows):
        spots = [pl.ds(t * lev_rows + level, members, stride=group) for t in range(tiles)]
        if raw_in:
            now = ens_ref[:, level, :]
        else:
            now = jnp.concatenate([rows_in[spot, :] for spot in spots], axis=1)
        centred = (now - jnp.sum(now, axis=0, keepdims=True) / members).astype(BF16)
        cross = jnp.dot(dev, centred, preferred_element_type=F32)
        height = jnp.concatenate([lev_s[level]] * tiles, axis=1)
        mixed = ((height * loc) * cross).astype(BF16)
        new = now + jnp.dot(gain, mixed, preferred_element_type=F32)
        if raw_out:
            out_ref[:, level, :] = new
        else:
            for t, spot in enumerate(spots):
                rows_out[spot, :] = new[:, t * LANES : (t + 1) * LANES]


def update(block, n_blocks, lev_rows, prior, values, variances, levels, olds, gathered, state):
    members = state.shape[0]
    n_obs = prior.shape[0]
    tiles = next(t for t in (6, 4, 2) if gathered.shape[1] % (t * LANES) == 0)
    group = tiles * lev_rows
    cols = gathered.shape[1]
    steps = cols // (tiles * LANES)
    raw_in, raw_out = block == 0, block == n_blocks - 1
    raw_spec = pl.BlockSpec((members, lev_rows, tiles * LANES), lambda i: (0, 0, i))
    row_spec = pl.BlockSpec((members, group, LANES), lambda i: (0, i, 0))
    out_dims = (members, lev_rows, cols) if raw_out else (members, steps * group, LANES)
    return pl.pallas_call(
        functools.partial(update_kernel, block, lev_rows, raw_in, raw_out),
        grid=(steps,),
        out_shape=[
            jax.ShapeDtypeStruct(out_dims, F32),
            jax.ShapeDtypeStruct(values.shape, F32),
        ],
        in_specs=[
            pl.BlockSpec((n_obs, LANES), lambda i: (0, 0)),
            pl.BlockSpec(values.shape, lambda i: (0, 0)),
            pl.BlockSpec(values.shape, lambda i: (0, 0)),
            pl.BlockSpec((None, lev_rows, n_obs), lambda i: (block, 0, 0)),
            pl.BlockSpec(olds.shape, lambda i: (0, 0)),
            pl.BlockSpec((n_obs, tiles * LANES), lambda i: (0, i)),
            raw_spec if raw_in else row_spec,
        ],
        out_specs=[
            raw_spec if raw_out else row_spec,
            pl.BlockSpec(values.shape, lambda i: (0, 0)),
        ],
        scratch_shapes=[pltpu.VMEM((n_obs, LANES), BF16), pltpu.VMEM((LANES, n_obs), BF16), pltpu.VMEM((lev_rows, n_obs, LANES), F32)],
        compiler_params=pltpu.CompilerParams(dimension_semantics=("arbitrary",)),
        name="update",
    )(prior, values, variances, levels, olds, gathered, state)


def solution(mesh):
    n_slab, n_lev = mesh.shape["slab"], mesh.shape["lev"]

    def on_device(ensemble, obs_cell, obs_value, obs_var, obs_frac, loc_column, loc_level):
        members, lev_rows, cols = ensemble.shape
        n_blocks = obs_cell.shape[0]
        state = ensemble
        means, heights = obs_value, loc_level.transpose(0, 2, 1)
        for block in range(n_blocks):
            flat = state if block == 0 else state.reshape(members * cols // LANES * lev_rows, LANES)
            part = pick(block, n_slab, members, lev_rows, obs_cell, obs_frac, flat)
            prior, gathered = exchange(block, n_slab, n_lev, part, loc_column)
            state, means = update(block, n_blocks, lev_rows, prior, obs_value, obs_var, heights, means, gathered, state)
        return state, means

    in_specs = (
        P(None, "lev", "slab"), P(), P(), P(), P(),
        P(None, "lev", "slab"), P(None, None, "lev"),
    )
    return jax.shard_map(
        on_device, mesh=mesh, in_specs=in_specs,
        out_specs=(P(None, "lev", "slab"), P()), check_vma=False,
    )
```

```python
import functools

import jax
import jax.numpy as jnp
from jax import lax
from jax.experimental import pallas as pl
from jax.experimental.pallas import tpu as pltpu
from jax.sharding import PartitionSpec as P

MESH = pl.DeviceIdType.MESH
LANES = 128
F32 = jnp.float32
BF16 = jnp.bfloat16
COST = pl.CostEstimate(flops=0, bytes_accessed=40_000_000, transcendentals=0)


def pick_kernel(block, members, lev_rows, n_slab, cell_ref, frac_ref, ens_ref, out_ref, acc, list_ref):
    n_obs = cell_ref.shape[1]
    raw = len(ens_ref.shape) == 3
    tiles = ens_ref.shape[2] // LANES if raw else ens_ref.shape[0] // (members * lev_rows)
    slab_cols = tiles * LANES
    total = slab_cols * n_slab
    base = lax.axis_index("lev") * (lev_rows * total)
    col_base = lax.axis_index("slab") * slab_cols
    acc[...] = jnp.zeros_like(acc)
    lane_ids = lax.broadcasted_iota(jnp.int32, (members, LANES), 1)

    def place(j):
        rest = cell_ref[block, j] - base
        row = jnp.int32(0)
        for level in range(1, lev_rows):
            row = row + (rest >= level * total).astype(jnp.int32)
        col = rest - row * total
        following = jnp.where(col + 1 == total, 0, col + 1)
        first, second = col - col_base, following - col_base
        in_band = (rest >= 0) & (rest < lev_rows * total)
        has_first = in_band & (first >= 0) & (first < slab_cols)
        has_second = in_band & (second >= 0) & (second < slab_cols)
        return row, first, second, has_first, has_second

    def scan(j, count):
        _, _, _, has_first, has_second = place(j)
        list_ref[count] = j
        return count + (has_first | has_second).astype(jnp.int32)

    count = lax.fori_loop(0, n_obs, scan, jnp.int32(0), unroll=8)

    def body(at, carry):
        j = list_ref[at]
        row, first, second, has_first, has_second = place(j)
        frac = frac_ref[block, j]
        tile_at = lax.shift_right_logical(j, 7)
        lane_at = j & (LANES - 1)

        def share(local, weight, mine, level):
            local = jnp.where(mine, local, 0)
            tile = lax.shift_right_logical(local, 7)
            if raw:
                window = ens_ref[:, level, pl.ds(pl.multiple_of(tile * LANES, LANES), LANES)]
            else:
                window = ens_ref[pl.ds(tile * lev_rows + row, members, stride=tiles * lev_rows), :]
            moved = pltpu.roll(window, (lane_at - (local & (LANES - 1))) & (LANES - 1), 1)
            return moved * jnp.where(mine, weight, 0.0)

        def put(level):
            value = share(first, 1.0 - frac, has_first, level) + share(second, frac, has_second, level)
            old = acc[tile_at, :members, :]
            acc[tile_at, :members, :] = jnp.where(lane_ids == lane_at, value, old)

        if raw:
            for level in range(lev_rows):
                pl.when(row == level)(functools.partial(put, level))
        else:
            put(0)
        return carry

    lax.fori_loop(0, count, body, 0)
    for t in range(n_obs // LANES):
        out_ref[t * LANES : (t + 1) * LANES, :] = acc[t].T


def pick(block, n_slab, members, lev_rows, cells, fracs, flat):
    n_obs = cells.shape[1]
    return pl.pallas_call(
        functools.partial(pick_kernel, block, members, lev_rows, n_slab),
        out_shape=jax.ShapeDtypeStruct((n_obs, LANES), F32),
        in_specs=[
            pl.BlockSpec(memory_space=pltpu.SMEM),
            pl.BlockSpec(memory_space=pltpu.SMEM),
            pl.BlockSpec(memory_space=pltpu.VMEM),
        ],
        out_specs=pl.BlockSpec(memory_space=pltpu.VMEM),
        scratch_shapes=[pltpu.VMEM((n_obs // LANES, LANES, LANES), F32), pltpu.SMEM((n_obs + 1,), jnp.int32)],
        cost_estimate=COST,
        name="pick",
    )(cells, fracs, flat)


def exchange_kernel(n_slab, n_lev, part_ref, prior_ref, landed, own, scat_send, scat_recv, cast_send, cast_recv):
    n = n_slab * n_lev
    me = lax.axis_index("slab") * n_lev + lax.axis_index("lev")

    def peer(k):
        p = lax.rem(me + k, n)
        return p, (p // n_lev, lax.rem(p, n_lev))

    def each(act):
        def body(k, c):
            act(k)
            return c
        lax.fori_loop(1, n, body, 0)

    barrier = pltpu.get_barrier_semaphore()
    each(lambda k: pl.semaphore_signal(barrier, inc=1, device_id=peer(k)[1], device_id_type=MESH))
    pl.semaphore_wait(barrier, n - 1)

    def scatter(k):
        p, where = peer(k)
        return pltpu.make_async_remote_copy(
            src_ref=part_ref.at[p], dst_ref=landed.at[k], send_sem=scat_send.at[k],
            recv_sem=scat_recv.at[k], device_id=where, device_id_type=MESH)

    def cast(k):
        return pltpu.make_async_remote_copy(
            src_ref=own, dst_ref=prior_ref.at[me], send_sem=cast_send.at[k],
            recv_sem=cast_recv.at[k], device_id=peer(k)[1], device_id_type=MESH)

    each(lambda k: scatter(k).start())
    landed[0] = part_ref[me]
    each(lambda k: scatter(k).wait_recv())
    own[...] = jnp.sum(landed[...], axis=0)
    each(lambda k: cast(k).start())
    prior_ref[me] = own[...]
    each(lambda k: scatter(k).wait_send())
    each(lambda k: cast(k).wait_recv())
    each(lambda k: cast(k).wait_send())


def exchange(block, n_slab, n_lev, part):
    n = n_slab * n_lev
    n_obs = part.shape[0]
    per = n_obs // n
    prior = pl.pallas_call(
        functools.partial(exchange_kernel, n_slab, n_lev),
        out_shape=jax.ShapeDtypeStruct((n, per, LANES), F32),
        in_specs=[pl.BlockSpec(memory_space=pltpu.VMEM)],
        out_specs=pl.BlockSpec(memory_space=pltpu.VMEM),
        scratch_shapes=[
            pltpu.VMEM((n, per, LANES), F32),
            pltpu.VMEM((per, LANES), F32),
            pltpu.SemaphoreType.DMA((n,)),
            pltpu.SemaphoreType.DMA((n,)),
            pltpu.SemaphoreType.DMA((n,)),
            pltpu.SemaphoreType.DMA((n,)),
        ],
        compiler_params=pltpu.CompilerParams(collective_id=block, has_side_effects=True),
        cost_estimate=COST,
        name="exchange",
    )(part.reshape(n, per, LANES))
    return prior.reshape(n_obs, LANES)


def update_kernel(block, lev_rows, raw_in, raw_out, prior_ref, value_ref, var_ref, lev_ref, old_ref, loc_ref, ens_ref, out_ref, mean_ref, dev_s, gain_s, lev_s):
    members = ens_ref.shape[0]
    n_obs = prior_ref.shape[0]
    tiles = loc_ref.shape[1] // LANES
    group = tiles * lev_rows

    @pl.when(pl.program_id(0) == 0)
    def _():
        def column(ref):
            return jnp.broadcast_to(ref[block : block + 1, :], (8, n_obs)).T[:, :1]

        value, var = column(value_ref), column(var_ref)
        prior = prior_ref[...]
        live = lax.broadcasted_iota(jnp.int32, prior.shape, 1) < members
        mean = jnp.sum(jnp.where(live, prior, 0.0), axis=1, keepdims=True) / members
        deviation = jnp.where(live, prior - mean, 0.0)
        spread = jnp.sum(deviation * deviation, axis=1, keepdims=True) / (members - 1.0)
        total = spread + var
        shrink = 1.0 / (1.0 + jnp.sqrt(var / total))
        gain = ((value - mean) - deviation * shrink) / (total * (members - 1.0))
        dev_s[...] = deviation.astype(BF16)
        gain_s[...] = gain.T.astype(BF16)
        mean_ref[...] = old_ref[...]
        mean_ref[block : block + 1, :] = jnp.broadcast_to(mean, (n_obs, LANES)).T[:1, :]
        for level in range(lev_rows):
            lev_s[level] = jnp.broadcast_to(lev_ref[level : level + 1, :], (LANES, n_obs)).T

    dev = dev_s[:, :members]
    gain = gain_s[:members, :]
    rows_in = None if raw_in else ens_ref.reshape(members * group, LANES)
    rows_out = None if raw_out else out_ref.reshape(members * group, LANES)
    loc = loc_ref[...].astype(F32)
    for level in range(lev_rows):
        spots = [pl.ds(t * lev_rows + level, members, stride=group) for t in range(tiles)]
        if raw_in:
            now = ens_ref[:, level, :]
        else:
            now = jnp.concatenate([rows_in[spot, :] for spot in spots], axis=1)
        centred = (now - jnp.sum(now, axis=0, keepdims=True) / members).astype(BF16)
        cross = jnp.dot(dev, centred, preferred_element_type=F32)
        height = jnp.concatenate([lev_s[level]] * tiles, axis=1)
        mixed = ((height * loc) * cross).astype(BF16)
        new = now + jnp.dot(gain, mixed, preferred_element_type=F32)
        if raw_out:
            out_ref[:, level, :] = new
        else:
            for t, spot in enumerate(spots):
                rows_out[spot, :] = new[:, t * LANES : (t + 1) * LANES]


def update(block, n_blocks, lev_rows, prior, values, variances, levels, olds, gathered, state):
    members = state.shape[0]
    n_obs = prior.shape[0]
    tiles = next(t for t in (6, 4, 2) if gathered.shape[1] % (t * LANES) == 0)
    group = tiles * lev_rows
    cols = gathered.shape[1]
    steps = cols // (tiles * LANES)
    raw_in, raw_out = block == 0, block == n_blocks - 1
    raw_spec = pl.BlockSpec((members, lev_rows, tiles * LANES), lambda i: (0, 0, i))
    row_spec = pl.BlockSpec((members, group, LANES), lambda i: (0, i, 0))
    out_dims = (members, lev_rows, cols) if raw_out else (members, steps * group, LANES)
    return pl.pallas_call(
        functools.partial(update_kernel, block, lev_rows, raw_in, raw_out),
        grid=(steps,),
        out_shape=[
            jax.ShapeDtypeStruct(out_dims, F32),
            jax.ShapeDtypeStruct(values.shape, F32),
        ],
        in_specs=[
            pl.BlockSpec((n_obs, LANES), lambda i: (0, 0)),
            pl.BlockSpec(values.shape, lambda i: (0, 0)),
            pl.BlockSpec(values.shape, lambda i: (0, 0)),
            pl.BlockSpec((None, lev_rows, n_obs), lambda i: (block, 0, 0)),
            pl.BlockSpec(olds.shape, lambda i: (0, 0)),
            pl.BlockSpec((n_obs, tiles * LANES), lambda i: (0, i)),
            raw_spec if raw_in else row_spec,
        ],
        out_specs=[
            raw_spec if raw_out else row_spec,
            pl.BlockSpec(values.shape, lambda i: (0, 0)),
        ],
        scratch_shapes=[pltpu.VMEM((n_obs, LANES), BF16), pltpu.VMEM((LANES, n_obs), BF16), pltpu.VMEM((lev_rows, n_obs, LANES), F32)],
        compiler_params=pltpu.CompilerParams(dimension_semantics=("arbitrary",)),
        cost_estimate=COST,
        name="update",
    )(prior, values, variances, levels, olds, gathered, state)


def solution(mesh):
    n_slab, n_lev = mesh.shape["slab"], mesh.shape["lev"]

    def on_device(ensemble, obs_cell, obs_value, obs_var, obs_frac, loc_column, loc_level):
        members, lev_rows, cols = ensemble.shape
        n_blocks = obs_cell.shape[0]
        state = ensemble
        means, heights = obs_value, loc_level.transpose(0, 2, 1)
        gathered = [lax.all_gather(loc_column[b], "lev", axis=0, tiled=True) for b in range(n_blocks)]
        for block in range(n_blocks):
            flat = state if block == 0 else state.reshape(members * cols // LANES * lev_rows, LANES)
            part = pick(block, n_slab, members, lev_rows, obs_cell, obs_frac, flat)
            prior = exchange(block, n_slab, n_lev, part)
            state, means = update(block, n_blocks, lev_rows, prior, obs_value, obs_var, heights, means, gathered[block], state)
        return state, means

    in_specs = (
        P(None, "lev", "slab"), P(), P(), P(), P(),
        P(None, "lev", "slab"), P(None, None, "lev"),
    )
    return jax.shard_map(
        on_device, mesh=mesh, in_specs=in_specs,
        out_specs=(P(None, "lev", "slab"), P()), check_vma=False,
    )
```

```python
import functools

import jax
import jax.numpy as jnp
from jax import lax
from jax.experimental import pallas as pl
from jax.experimental.pallas import tpu as pltpu
from jax.sharding import PartitionSpec as P

MESH = pl.DeviceIdType.MESH
LANES = 128
F32 = jnp.float32
BF16 = jnp.bfloat16


def pick_kernel(block, members, lev_rows, n_slab, cell_ref, frac_ref, ens_ref, out_ref, acc, list_ref):
    n_obs = cell_ref.shape[1]
    raw = len(ens_ref.shape) == 3
    tiles = ens_ref.shape[2] // LANES if raw else ens_ref.shape[0] // (members * lev_rows)
    slab_cols = tiles * LANES
    total = slab_cols * n_slab
    base = lax.axis_index("lev") * (lev_rows * total)
    col_base = lax.axis_index("slab") * slab_cols
    acc[...] = jnp.zeros_like(acc)
    lane_ids = lax.broadcasted_iota(jnp.int32, (members, LANES), 1)

    def place(j):
        rest = cell_ref[block, j] - base
        row = jnp.int32(0)
        for level in range(1, lev_rows):
            row = row + (rest >= level * total).astype(jnp.int32)
        col = rest - row * total
        following = jnp.where(col + 1 == total, 0, col + 1)
        first, second = col - col_base, following - col_base
        in_band = (rest >= 0) & (rest < lev_rows * total)
        has_first = in_band & (first >= 0) & (first < slab_cols)
        has_second = in_band & (second >= 0) & (second < slab_cols)
        return row, first, second, has_first, has_second

    def scan(j, count):
        _, _, _, has_first, has_second = place(j)
        list_ref[count] = j
        return count + (has_first | has_second).astype(jnp.int32)

    count = lax.fori_loop(0, n_obs, scan, jnp.int32(0), unroll=8)

    def body(at, carry):
        j = list_ref[at]
        row, first, second, has_first, has_second = place(j)
        frac = frac_ref[block, j]
        tile_at = lax.shift_right_logical(j, 7)
        lane_at = j & (LANES - 1)

        def share(local, weight, mine, level):
            local = jnp.where(mine, local, 0)
            tile = lax.shift_right_logical(local, 7)
            if raw:
                window = ens_ref[:, level, pl.ds(pl.multiple_of(tile * LANES, LANES), LANES)]
            else:
                window = ens_ref[pl.ds(tile * lev_rows + row, members, stride=tiles * lev_rows), :]
            moved = pltpu.roll(window, (lane_at - (local & (LANES - 1))) & (LANES - 1), 1)
            return moved * jnp.where(mine, weight, 0.0)

        def put(level):
            value = share(first, 1.0 - frac, has_first, level) + share(second, frac, has_second, level)
            old = acc[tile_at, :members, :]
            acc[tile_at, :members, :] = jnp.where(lane_ids == lane_at, value, old)

        if raw:
            for level in range(lev_rows):
                pl.when(row == level)(functools.partial(put, level))
        else:
            put(0)
        return carry

    lax.fori_loop(0, count, body, 0)
    for t in range(n_obs // LANES):
        out_ref[t * LANES : (t + 1) * LANES, :] = acc[t].T


def pick(block, n_slab, members, lev_rows, cells, fracs, flat):
    n_obs = cells.shape[1]
    return pl.pallas_call(
        functools.partial(pick_kernel, block, members, lev_rows, n_slab),
        out_shape=jax.ShapeDtypeStruct((n_obs, LANES), F32),
        in_specs=[
            pl.BlockSpec(memory_space=pltpu.SMEM),
            pl.BlockSpec(memory_space=pltpu.SMEM),
            pl.BlockSpec(memory_space=pltpu.VMEM),
        ],
        out_specs=pl.BlockSpec(memory_space=pltpu.VMEM),
        scratch_shapes=[pltpu.VMEM((n_obs // LANES, LANES, LANES), F32), pltpu.SMEM((n_obs + 1,), jnp.int32)],
        name="pick",
    )(cells, fracs, flat)


def exchange_kernel(
    n_slab, n_lev, pieces, part_ref, loc_ref, prior_ref, gat_ref, landed, own,
    scat_send, scat_recv, cast_send, cast_recv, up_send, down_send, line_recv,
):
    n = n_slab * n_lev
    slab, lev = lax.axis_index("slab"), lax.axis_index("lev")
    me = slab * n_lev + lev
    rows = loc_ref.shape[1]
    cut = rows // pieces

    def peer(k):
        p = lax.rem(me + k, n)
        return p, (p // n_lev, lax.rem(p, n_lev))

    barrier = pltpu.get_barrier_semaphore()

    def greet(k, c):
        _, where = peer(k)
        pl.semaphore_signal(barrier, inc=1, device_id=where, device_id_type=MESH)
        return c

    lax.fori_loop(1, n, greet, 0)
    pl.semaphore_wait(barrier, n - 1)

    def scatter(k):
        p, where = peer(k)
        return pltpu.make_async_remote_copy(
            src_ref=part_ref.at[p], dst_ref=landed.at[k], send_sem=scat_send.at[k],
            recv_sem=scat_recv.at[k], device_id=where, device_id_type=MESH)

    def cast(k):
        _, where = peer(k)
        return pltpu.make_async_remote_copy(
            src_ref=own, dst_ref=prior_ref.at[me], send_sem=cast_send.at[k],
            recv_sem=cast_recv.at[k], device_id=where, device_id_type=MESH)

    def each(act):
        def body(k, c):
            act(k)
            return c
        lax.fori_loop(1, n, body, 0)

    def slot(source, h):
        return gat_ref.at[pl.ds(pl.multiple_of(source * rows + h * cut, cut), cut), :]

    def hop(source, h, first, step):
        src = loc_ref.at[0, pl.ds(h * cut, cut), :] if first else slot(source, h)
        sems = up_send if step > 0 else down_send
        return pltpu.make_async_remote_copy(
            src_ref=src, dst_ref=slot(source, h), send_sem=sems.at[source, h],
            recv_sem=line_recv.at[source, h], device_id=(slab, lev + step), device_id_type=MESH)

    each(lambda k: scatter(k).start())
    for h in range(pieces):
        @pl.when(lev < n_lev - 1)
        def _():
            hop(lev, h, True, 1).start()

        @pl.when(lev > 0)
        def _():
            hop(lev, h, True, -1).start()

    gat_ref[pl.ds(pl.multiple_of(lev * rows, rows), rows), :] = loc_ref[0]

    each(lambda k: scatter(k).wait_recv())
    landed[0] = part_ref[me]
    own[...] = jnp.sum(landed[...], axis=0)
    each(lambda k: cast(k).start())
    prior_ref[me] = own[...]

    for s in range(1, n_lev):
        for h in range(pieces):
            @pl.when(lev - s >= 0)
            def _():
                hop(lev - s, h, False, 1).wait_recv()

                @pl.when(lev < n_lev - 1)
                def _():
                    hop(lev - s, h, False, 1).start()

            @pl.when(lev + s <= n_lev - 1)
            def _():
                hop(lev + s, h, False, -1).wait_recv()

                @pl.when(lev > 0)
                def _():
                    hop(lev + s, h, False, -1).start()

    each(lambda k: cast(k).wait_recv())
    each(lambda k: scatter(k).wait_send())
    each(lambda k: cast(k).wait_send())
    for s in range(n_lev):
        for h in range(pieces):
            @pl.when((lev - s >= 0) & (lev < n_lev - 1))
            def _():
                hop(lev - s, h, s == 0, 1).wait_send()

            @pl.when((lev + s <= n_lev - 1) & (lev > 0))
            def _():
                hop(lev + s, h, s == 0, -1).wait_send()


def exchange(block, n_slab, n_lev, part, loc):
    n = n_slab * n_lev
    n_obs = part.shape[0]
    per = n_obs // n
    rows, cols = loc.shape[1:]
    pieces = 2
    prior, gathered = pl.pallas_call(
        functools.partial(exchange_kernel, n_slab, n_lev, pieces),
        grid=(1,),
        out_shape=[
            jax.ShapeDtypeStruct((n, per, LANES), F32),
            jax.ShapeDtypeStruct((n_obs, cols), BF16),
        ],
        in_specs=[
            pl.BlockSpec((n, per, LANES), lambda i: (0, 0, 0)),
            pl.BlockSpec((1, rows, cols), lambda i: (block, 0, 0)),
        ],
        out_specs=[
            pl.BlockSpec((n, per, LANES), lambda i: (0, 0, 0)),
            pl.BlockSpec((n_obs, cols), lambda i: (0, 0)),
        ],
        scratch_shapes=[
            pltpu.VMEM((n, per, LANES), F32),
            pltpu.VMEM((per, LANES), F32),
            pltpu.SemaphoreType.DMA((n,)),
            pltpu.SemaphoreType.DMA((n,)),
            pltpu.SemaphoreType.DMA((n,)),
            pltpu.SemaphoreType.DMA((n,)),
            pltpu.SemaphoreType.DMA((n_lev, pieces)),
            pltpu.SemaphoreType.DMA((n_lev, pieces)),
            pltpu.SemaphoreType.DMA((n_lev, pieces)),
        ],
        compiler_params=pltpu.CompilerParams(collective_id=block, has_side_effects=True),
        name="exchange",
    )(part.reshape(n, per, LANES), loc)
    return prior.reshape(n_obs, LANES), gathered


def update_kernel(block, lev_rows, raw_in, raw_out, prior_ref, value_ref, var_ref, lev_ref, old_ref, loc_ref, ens_ref, out_ref, mean_ref, dev_s, gain_s, lev_s):
    members = ens_ref.shape[0]
    n_obs = prior_ref.shape[0]
    tiles = loc_ref.shape[1] // LANES
    group = tiles * lev_rows

    @pl.when(pl.program_id(0) == 0)
    def _():
        def column(ref):
            return jnp.broadcast_to(ref[block : block + 1, :], (8, n_obs)).T[:, :1]

        value, var = column(value_ref), column(var_ref)
        prior = prior_ref[...]
        live = lax.broadcasted_iota(jnp.int32, prior.shape, 1) < members
        mean = jnp.sum(jnp.where(live, prior, 0.0), axis=1, keepdims=True) / members
        deviation = jnp.where(live, prior - mean, 0.0)
        spread = jnp.sum(deviation * deviation, axis=1, keepdims=True) / (members - 1.0)
        total = spread + var
        shrink = 1.0 / (1.0 + jnp.sqrt(var / total))
        gain = ((value - mean) - deviation * shrink) / (total * (members - 1.0))
        dev_s[...] = deviation.astype(BF16)
        gain_s[...] = gain.T.astype(BF16)
        mean_ref[...] = old_ref[...]
        mean_ref[block : block + 1, :] = jnp.broadcast_to(mean, (n_obs, LANES)).T[:1, :]
        for level in range(lev_rows):
            lev_s[level] = jnp.broadcast_to(lev_ref[level : level + 1, :], (LANES, n_obs)).T

    dev = dev_s[:, :members]
    gain = gain_s[:members, :]
    rows_in = None if raw_in else ens_ref.reshape(members * group, LANES)
    rows_out = None if raw_out else out_ref.reshape(members * group, LANES)
    loc = loc_ref[...].astype(F32)
    for level in range(lev_rows):
        spots = [pl.ds(t * lev_rows + level, members, stride=group) for t in range(tiles)]
        if raw_in:
            now = ens_ref[:, level, :]
        else:
            now = jnp.concatenate([rows_in[spot, :] for spot in spots], axis=1)
        centred = (now - jnp.sum(now, axis=0, keepdims=True) / members).astype(BF16)
        cross = jnp.dot(dev, centred, preferred_element_type=F32)
        height = jnp.concatenate([lev_s[level]] * tiles, axis=1)
        mixed = ((height * loc) * cross).astype(BF16)
        new = now + jnp.dot(gain, mixed, preferred_element_type=F32)
        if raw_out:
            out_ref[:, level, :] = new
        else:
            for t, spot in enumerate(spots):
                rows_out[spot, :] = new[:, t * LANES : (t + 1) * LANES]


def update(block, n_blocks, lev_rows, prior, values, variances, levels, olds, gathered, state):
    members = state.shape[0]
    n_obs = prior.shape[0]
    tiles = next(t for t in (6, 4, 2) if gathered.shape[1] % (t * LANES) == 0)
    group = tiles * lev_rows
    cols = gathered.shape[1]
    steps = cols // (tiles * LANES)
    raw_in, raw_out = block == 0, block == n_blocks - 1
    raw_spec = pl.BlockSpec((members, lev_rows, tiles * LANES), lambda i: (0, 0, i))
    row_spec = pl.BlockSpec((members, group, LANES), lambda i: (0, i, 0))
    out_dims = (members, lev_rows, cols) if raw_out else (members, steps * group, LANES)
    return pl.pallas_call(
        functools.partial(update_kernel, block, lev_rows, raw_in, raw_out),
        grid=(steps,),
        out_shape=[
            jax.ShapeDtypeStruct(out_dims, F32),
            jax.ShapeDtypeStruct(values.shape, F32),
        ],
        in_specs=[
            pl.BlockSpec((n_obs, LANES), lambda i: (0, 0)),
            pl.BlockSpec(values.shape, lambda i: (0, 0)),
            pl.BlockSpec(values.shape, lambda i: (0, 0)),
            pl.BlockSpec((None, lev_rows, n_obs), lambda i: (block, 0, 0)),
            pl.BlockSpec(olds.shape, lambda i: (0, 0)),
            pl.BlockSpec((n_obs, tiles * LANES), lambda i: (0, i)),
            raw_spec if raw_in else row_spec,
        ],
        out_specs=[
            raw_spec if raw_out else row_spec,
            pl.BlockSpec(values.shape, lambda i: (0, 0)),
        ],
        scratch_shapes=[pltpu.VMEM((n_obs, LANES), BF16), pltpu.VMEM((LANES, n_obs), BF16), pltpu.VMEM((lev_rows, n_obs, LANES), F32)],
        compiler_params=pltpu.CompilerParams(dimension_semantics=("arbitrary",)),
        name="update",
    )(prior, values, variances, levels, olds, gathered, state)


def solution(mesh):
    n_slab, n_lev = mesh.shape["slab"], mesh.shape["lev"]

    def on_device(ensemble, obs_cell, obs_value, obs_var, obs_frac, loc_column, loc_level):
        members, lev_rows, cols = ensemble.shape
        n_blocks = obs_cell.shape[0]
        state = ensemble
        means, heights = obs_value, loc_level.transpose(0, 2, 1)
        for block in range(n_blocks):
            flat = state if block == 0 else state.reshape(members * cols // LANES * lev_rows, LANES)
            part = pick(block, n_slab, members, lev_rows, obs_cell, obs_frac, flat)
            prior, gathered = exchange(block, n_slab, n_lev, part, loc_column)
            state, means = update(block, n_blocks, lev_rows, prior, obs_value, obs_var, heights, means, gathered, state)
        return state, means

    in_specs = (
        P(None, "lev", "slab"), P(), P(), P(), P(),
        P(None, "lev", "slab"), P(None, None, "lev"),
    )
    return jax.shard_map(
        on_device, mesh=mesh, in_specs=in_specs,
        out_specs=(P(None, "lev", "slab"), P()), check_vma=False,
    )
```
